32 devices in a mesh: blk: 8 (over z, x), bfly: 4 (over y, core).
Axes of the slice: x: 2, y: 2, z: 4, core: 2. Of those that a mesh axis runs over, the one named last changes fastest.
Arguments:
- port_vectors: bfloat16 [8, 4, 768, 128], P('blk', 'bfly'), may hold values from -6 to 6
- column_leaf: bfloat16 [8, 4, 384, 768], P('blk', 'bfly'), may hold values from -0.21875 to 0.21875
- transfer: bfloat16 [8, 4, 4, 384, 768], P('blk', None, 'bfly'), may hold values from -0.21875 to 0.21875
- row_leaf: bfloat16 [8, 4, 768, 384], P('blk', 'bfly'), may hold values from -0.3125 to 0.3125
Outputs:
- field: bfloat16 [4, 768, 128], P('bfly', 'blk')
The draws below stay inside these ranges and needn't reach their ends.
All inputs are finite; a program needn't handle non-finite values.
Results may differ from the reference program's by a relative error of at most 0.0095.
Values may be sent and summed in bfloat16 or wider, within the bound.
A program may use at most 64 MiB of HBM per device.

```python
import math
import jax
import jax.numpy as jnp
import numpy as np
from jax import lax

RANK = 384
LEAF = 768
PORTS = 128
LEVELS = 4
BLOCKS = 8
N_BLK = 8
N_BFLY = 4


def steps_of(stream_key, dims, pieces, smallest, high):
    gain = 1.0
    for axis_at, parts in pieces:
        steps = jax.random.uniform(jax.random.fold_in(jax.random.fold_in(stream_key, 6), axis_at), (parts,), jnp.float32, smallest / len(pieces), high / len(pieces))
        gain = gain * jnp.repeat(jnp.exp(steps), dims[axis_at] // parts).reshape((-1,) + (1,) * (len(dims) - 1 - axis_at))
    return gain


def bell_draw(rng, shape, scale, reach, split=(), kind=jnp.bfloat16):
    array = scale * jax.random.normal(rng, shape, jnp.float32)
    if split:
        array = array * steps_of(rng, shape, split, -0.22, 0.18)
    return jnp.clip(array, -reach, reach).astype(kind)


def setup_inputs(seed: int = 0) -> dict:
    seeds = jax.random.split(jax.random.key(seed), 5)
    return {
        "port_vectors": bell_draw(seeds[0], (BLOCKS, N_BFLY, LEAF, PORTS), 1.0, 6.0, ((0, 8), (1, 4))),
        "column_leaf": bell_draw(seeds[1], (BLOCKS, N_BFLY, RANK, LEAF), LEAF ** -0.5, 0.21875, ((0, 8), (1, 4))),
        "transfer": bell_draw(seeds[2], (BLOCKS, LEVELS, N_BFLY, RANK, 2 * RANK), (2 * RANK) ** -0.5, 0.21875, ((0, 8), (2, 4))),
        "row_leaf": bell_draw(seeds[3], (BLOCKS, N_BFLY, LEAF, RANK), RANK ** -0.5, 0.3125, ((0, 8), (1, 4))),
    }


def reference(port_vectors, column_leaf, transfer, row_leaf):
    bit_count = N_BFLY.bit_length() - 1
    positions = np.arange(N_BFLY)

    def one_block(total, items):
        ports, cleaf, trans, rleaf = items
        state = jnp.einsum('pkl,plr->pkr', cleaf.astype(jnp.float32), ports.astype(jnp.float32)).astype(jnp.bfloat16)
        for level in range(LEVELS):
            stride = 1 << level % bit_count
            lower = jnp.asarray(positions & ~stride, dtype=jnp.int32)
            upper = jnp.asarray(positions | stride, dtype=jnp.int32)
            stacked = jnp.concatenate([state[lower], state[upper]], axis=1)
            state = jnp.einsum('pkj,pjr->pkr', trans[level].astype(jnp.float32), stacked.astype(jnp.float32)).astype(jnp.bfloat16)
        partial_rows = jnp.einsum('plk,pkr->plr', rleaf.astype(jnp.float32), state.astype(jnp.float32))
        return (total + partial_rows, None)
    start = jnp.zeros((N_BFLY, LEAF, PORTS), jnp.float32)
    total, _ = lax.scan(one_block, start, (port_vectors, column_leaf, transfer, row_leaf))
    return (total * (1.0 / math.sqrt(N_BLK))).astype(jnp.bfloat16)
```

```python
import functools
import math

import jax
import jax.numpy as jnp
from jax import lax
from jax.experimental import pallas as pl
from jax.experimental.pallas import tpu as pltpu
from jax.sharding import PartitionSpec as P

MESH = pl.DeviceIdType.MESH


def kernel(
    n_blk, n_bfly,
    ports_hbm, column_hbm, transfer_hbm, row_hbm, out_ref,
    ports, column, transfer, row, stacked, outgoing, incoming,
    load_sem, send_sem, recv_sem, scatter_sem, gather_sem,
):
    levels, rank, _ = transfer.shape
    owned = outgoing.shape[1]
    bit_count = n_bfly.bit_length() - 1
    block = lax.axis_index("blk")
    position = lax.axis_index("bfly")

    loads = [
        pltpu.make_async_copy(ports_hbm.at[0, 0], ports, load_sem.at[0]),
        pltpu.make_async_copy(column_hbm.at[0, 0], column, load_sem.at[1]),
    ]
    for level in range(levels):
        loads.append(
            pltpu.make_async_copy(
                transfer_hbm.at[0, level, 0], transfer.at[level], load_sem.at[2 + level]
            )
        )
    loads.append(pltpu.make_async_copy(row_hbm.at[0, 0], row, load_sem.at[2 + levels]))
    for load in loads:
        load.start()

    bits = [(position // 2**bit) % 2 for bit in range(bit_count)]
    partners = [position + (1 - 2 * bits[bit]) * 2**bit for bit in range(bit_count)]
    barrier = pltpu.get_barrier_semaphore()
    for bit in range(min(bit_count, levels)):
        pl.semaphore_signal(
            barrier, inc=1, device_id={"bfly": partners[bit]}, device_id_type=MESH
        )
    for step in range(1, n_blk):
        pl.semaphore_signal(
            barrier, inc=1, device_id={"blk": lax.rem(block + step, n_blk)}, device_id_type=MESH
        )

    loads[0].wait()
    loads[1].wait()
    state = jnp.dot(column[...], ports[...], preferred_element_type=jnp.float32)
    pl.semaphore_wait(barrier, min(bit_count, levels) + n_blk - 1)

    sends = []
    for level in range(levels):
        bit = level % bit_count
        mine = pl.ds(pl.multiple_of(bits[bit] * rank, rank), rank)
        other = pl.ds(pl.multiple_of((1 - bits[bit]) * rank, rank), rank)
        stacked[level, mine, :] = state.astype(jnp.bfloat16)
        copy = pltpu.make_async_remote_copy(
            src_ref=stacked.at[level, mine, :],
            dst_ref=stacked.at[level, mine, :],
            send_sem=send_sem.at[level],
            recv_sem=recv_sem.at[level],
            device_id={"bfly": partners[bit]},
            device_id_type=MESH,
        )
        copy.start()
        sends.append(copy)
        loads[2 + level].wait()
        state = jnp.dot(
            transfer[level, :, mine], stacked[level, mine, :],
            preferred_element_type=jnp.float32,
        )
        copy.wait_recv()
        state = state + jnp.dot(
            transfer[level, :, other], stacked[level, other, :],
            preferred_element_type=jnp.float32,
        )

    loads[2 + levels].wait()
    state = state.astype(jnp.bfloat16)
    partial = jnp.dot(row[...], state, preferred_element_type=jnp.float32)
    for index in range(n_blk):
        outgoing[index] = partial[index * owned : (index + 1) * owned].astype(jnp.bfloat16)
    for step in range(1, n_blk):
        target = lax.rem(block + step, n_blk)
        copy = pltpu.make_async_remote_copy(
            src_ref=outgoing.at[target],
            dst_ref=incoming.at[step],
            send_sem=scatter_sem.at[step],
            recv_sem=gather_sem.at[step],
            device_id={"blk": target},
            device_id_type=MESH,
        )
        copy.start()
        sends.append(copy)
    total = outgoing[block].astype(jnp.float32)
    for step in range(1, n_blk):
        sends[levels + step - 1].wait_recv()
        total = total + incoming[step].astype(jnp.float32)
    out_ref[0] = (total * (1.0 / math.sqrt(n_blk))).astype(jnp.bfloat16)
    for copy in sends:
        copy.wait_send()


def solution(mesh):
    n_blk, n_bfly = mesh.shape["blk"], mesh.shape["bfly"]

    def local(port_vectors, column_leaf, transfer, row_leaf):
        _, _, leaf, ports = port_vectors.shape
        rank = column_leaf.shape[2]
        levels = transfer.shape[1]
        owned = row_leaf.shape[2] // n_blk
        bf16 = jnp.bfloat16
        return pl.pallas_call(
            functools.partial(kernel, n_blk, n_bfly),
            out_shape=jax.ShapeDtypeStruct((1, owned, ports), bf16),
            in_specs=[pl.BlockSpec(memory_space=pl.ANY)] * 4,
            out_specs=pl.BlockSpec(memory_space=pltpu.VMEM),
            scratch_shapes=[
                pltpu.VMEM((leaf, ports), bf16),
                pltpu.VMEM((rank, leaf), bf16),
                pltpu.VMEM((levels, rank, 2 * rank), bf16),
                pltpu.VMEM((row_leaf.shape[2], rank), bf16),
                pltpu.VMEM((levels, 2 * rank, ports), bf16),
                pltpu.VMEM((n_blk, owned, ports), bf16),
                pltpu.VMEM((n_blk, owned, ports), bf16),
                pltpu.SemaphoreType.DMA((3 + levels,)),
                pltpu.SemaphoreType.DMA((levels,)),
                pltpu.SemaphoreType.DMA((levels,)),
                pltpu.SemaphoreType.DMA((n_blk,)),
                pltpu.SemaphoreType.DMA((n_blk,)),
            ],
            compiler_params=pltpu.CompilerParams(collective_id=0, has_side_effects=True),
        )(port_vectors, column_leaf, transfer, row_leaf)

    placed = (
        P("blk", "bfly", None, None),
        P("blk", "bfly", None, None),
        P("blk", None, "bfly", None, None),
        P("blk", "bfly", None, None),
    )
    return jax.shard_map(
        local, mesh=mesh, in_specs=placed, out_specs=P("bfly", "blk", None), check_vma=False
    )
```

```python
import functools
import math

import jax
import jax.numpy as jnp
from jax import lax
from jax.experimental import pallas as pl
from jax.experimental.pallas import tpu as pltpu
from jax.sharding import PartitionSpec as P

PIECES = 2
MESH = pl.DeviceIdType.MESH


def kernel(
    n_blk, n_bfly, pieces,
    ports_hbm, column_hbm, transfer_hbm, row_hbm, out_ref,
    ports, column, transfer, row, stacked, outgoing, incoming, merged, partial,
    load_sem, send_sem, recv_sem, scatter_sem, gather_sem,
):
    levels, rank, _ = transfer.shape
    owned = outgoing.shape[1]
    bit_count = n_bfly.bit_length() - 1
    block = lax.axis_index("blk")
    position = lax.axis_index("bfly")

    loads = [
        pltpu.make_async_copy(ports_hbm.at[0, 0], ports, load_sem.at[0]),
        pltpu.make_async_copy(column_hbm.at[0, 0], column, load_sem.at[1]),
    ]
    for level in range(levels):
        loads.append(
            pltpu.make_async_copy(
                transfer_hbm.at[0, level, 0], transfer.at[level], load_sem.at[2 + level]
            )
        )
    loads.append(pltpu.make_async_copy(row_hbm.at[0, 0], row, load_sem.at[2 + levels]))
    for load in loads:
        load.start()

    bits = [(position // 2**bit) % 2 for bit in range(bit_count)]
    partners = [position + (1 - 2 * bits[bit]) * 2**bit for bit in range(bit_count)]
    barrier = pltpu.get_barrier_semaphore()
    for bit in range(min(bit_count, levels)):
        pl.semaphore_signal(
            barrier, inc=1, device_id={"bfly": partners[bit]}, device_id_type=MESH
        )
    for step in range(1, n_blk):
        pl.semaphore_signal(
            barrier, inc=1, device_id={"blk": lax.rem(block + step, n_blk)}, device_id_type=MESH
        )

    loads[0].wait()
    loads[1].wait()
    state = jnp.dot(column[...], ports[...], preferred_element_type=jnp.float32)
    pl.semaphore_wait(barrier, min(bit_count, levels) + n_blk - 1)

    sends = []
    width = ports.shape[1] // pieces
    spans = [pl.ds(piece * width, width) for piece in range(pieces)]

    def side(which):
        return pl.ds(pl.multiple_of(which * rank, rank), rank)

    def send(level, piece, value):
        mine = bits[level % bit_count]
        stacked[level, mine, spans[piece], :] = value.astype(jnp.bfloat16)
        copy = pltpu.make_async_remote_copy(
            src_ref=stacked.at[level, mine, spans[piece], :],
            dst_ref=stacked.at[level, mine, spans[piece], :],
            send_sem=send_sem.at[level, piece],
            recv_sem=recv_sem.at[level, piece],
            device_id={"bfly": partners[level % bit_count]},
            device_id_type=MESH,
        )
        copy.start()
        sends.append(copy)
        return copy

    def mix(level, which, piece):
        return lax.dot_general(
            stacked[level, which, spans[piece], :], transfer[level, :, side(which)],
            (((1,), (1,)), ((), ())), preferred_element_type=jnp.float32,
        )

    def rows(which):
        return lax.dot_general(
            merged[:, side(which)], stacked[levels - 1, which],
            (((1,), (1,)), ((), ())), preferred_element_type=jnp.float32,
        )

    first = state.T
    flying = [
        send(0, piece, first[piece * width : (piece + 1) * width]) for piece in range(pieces)
    ]
    for level in range(levels - 1):
        mine = bits[level % bit_count]
        if level == 0:
            loads[2].wait()
            begun = [mix(0, mine, piece) for piece in range(pieces)]
        loads[3 + level].wait()
        following, later = [], []
        for piece in range(pieces):
            flying[piece].wait_recv()
            mixed = begun[piece] + mix(level, 1 - mine, piece)
            following.append(send(level + 1, piece, mixed))
            if level + 1 < levels - 1:
                later.append(mix(level + 1, bits[(level + 1) % bit_count], piece))
        flying, begun = following, later
        if level == min(1, levels - 2):
            loads[2 + levels].wait()
    level = levels - 1
    mine = bits[level % bit_count]
    merged[...] = jnp.dot(
        row[...], transfer[level], preferred_element_type=jnp.float32
    ).astype(jnp.bfloat16)
    partial[...] = rows(mine)
    for copy in flying:
        copy.wait_recv()
    total = partial[...] + rows(1 - mine)
    for index in range(n_blk):
        outgoing[index] = total[index * owned : (index + 1) * owned].astype(jnp.bfloat16)
    for step in range(1, n_blk):
        target = lax.rem(block + step, n_blk)
        copy = pltpu.make_async_remote_copy(
            src_ref=outgoing.at[target],
            dst_ref=incoming.at[step],
            send_sem=scatter_sem.at[step],
            recv_sem=gather_sem.at[step],
            device_id={"blk": target},
            device_id_type=MESH,
        )
        copy.start()
        sends.append(copy)
    total = outgoing[block].astype(jnp.float32)
    for step in range(1, n_blk):
        sends[levels * pieces + step - 1].wait_recv()
        total = total + incoming[step].astype(jnp.float32)
    out_ref[0] = (total * (1.0 / math.sqrt(n_blk))).astype(jnp.bfloat16)
    for copy in sends:
        copy.wait_send()


def solution(mesh):
    n_blk, n_bfly = mesh.shape["blk"], mesh.shape["bfly"]

    def local(port_vectors, column_leaf, transfer, row_leaf):
        _, _, leaf, ports = port_vectors.shape
        rank = column_leaf.shape[2]
        levels = transfer.shape[1]
        owned = row_leaf.shape[2] // n_blk
        bf16 = jnp.bfloat16
        return pl.pallas_call(
            functools.partial(kernel, n_blk, n_bfly, PIECES),
            out_shape=pltpu.VMEM((1, owned, ports), bf16),
            in_specs=[pl.BlockSpec(memory_space=pl.ANY)] * 4,
            out_specs=pl.BlockSpec(memory_space=pltpu.VMEM),
            scratch_shapes=[
                pltpu.VMEM((leaf, ports), bf16),
                pltpu.VMEM((rank, leaf), bf16),
                pltpu.VMEM((levels, rank, 2 * rank), bf16),
                pltpu.VMEM((row_leaf.shape[2], rank), bf16),
                pltpu.VMEM((levels, 2, ports, rank), bf16),
                pltpu.VMEM((n_blk, owned, ports), bf16),
                pltpu.VMEM((n_blk, owned, ports), bf16),
                pltpu.VMEM((row_leaf.shape[2], 2 * rank), bf16),
                pltpu.VMEM((row_leaf.shape[2], ports), jnp.float32),
                pltpu.SemaphoreType.DMA((3 + levels,)),
                pltpu.SemaphoreType.DMA((levels, PIECES)),
                pltpu.SemaphoreType.DMA((levels, PIECES)),
                pltpu.SemaphoreType.DMA((n_blk,)),
                pltpu.SemaphoreType.DMA((n_blk,)),
            ],
            compiler_params=pltpu.CompilerParams(collective_id=0, has_side_effects=True),
        )(port_vectors, column_leaf, transfer, row_leaf)

    placed = (
        P("blk", "bfly", None, None),
        P("blk", "bfly", None, None),
        P("blk", None, "bfly", None, None),
        P("blk", "bfly", None, None),
    )
    return jax.shard_map(
        local, mesh=mesh, in_specs=placed, out_specs=P("bfly", "blk", None), check_vma=False
    )
```
